32 devices in a mesh: dp: 32 (over z, y, x, core), tensor: 1.
Axes of the slice: x: 2, y: 2, z: 4, core: 2. Of those that a mesh axis runs over, the one named last changes fastest.
Arguments:
- tokens: bfloat16 [4096, 2048], P('dp'), may hold values from -8 to 8
- grad_out: bfloat16 [4096, 2048], P('dp'), may hold values from -6 to 6
- route_ids: int32 [4096, 4], P('dp'), may hold values from 0 to 59, as said below
- expert_map: int32 [60], replicated, may hold values from 0 to 63, as said below
- router: bfloat16 [2048, 60], replicated, may hold values from -1 to 1
- shared_gate: bfloat16 [2048], replicated, may hold values from -0.125 to 0.125
- sh_gate: bfloat16 [2048, 2816], P('dp', 'tensor'), may hold values from -0.125 to 0.125
- sh_up: bfloat16 [2048, 2816], P('dp', 'tensor'), may hold values from -0.125 to 0.125
- sh_down: bfloat16 [2816, 2048], P('tensor', 'dp'), may hold values from -0.109375 to 0.109375
- ex_gate: bfloat16 [64, 2048, 1408], P('dp', None, 'tensor'), may hold values from -0.125 to 0.125
- ex_up: bfloat16 [64, 2048, 1408], P('dp', None, 'tensor'), may hold values from -0.125 to 0.125
- ex_down: bfloat16 [64, 1408, 2048], P('dp', 'tensor'), may hold values from -0.15625 to 0.15625
Outputs:
- mixed: bfloat16 [4096, 2048], P('dp', 'tensor')
- grad_tokens: bfloat16 [4096, 2048], P('dp', 'tensor')
The draws below stay inside these ranges and needn't reach their ends.
Inputs may be any that keep to these rules, and one draw needn't show every extreme that they name: `route_ids`: each row names 4 different experts. Within the rows of one device (aligned blocks of 128 rows), no expert is named more than 9 times over all 4 columns, and some expert is named exactly 9 times. Entries are distinct. Expert e uses the weights of slot expert_map[e]; slot s is held by index s // 2 of dp. Slots that no expert names are not used.
All inputs are finite; a program needn't handle non-finite values.
Results may differ from the reference program's by a relative error of at most 0.011.
Values may be sent and summed in bfloat16 or wider, within the bound.
No kernel may reach another device: no remote copies, remote signals or barrier semaphores. Data moves between devices by JAX's collectives and lax.ppermute only.
A program may use at most 128 MiB of HBM per device.

```python
import math
import jax
import jax.numpy as jnp
from jax import lax

D = 2048
F = 1408
EXPERTS = 60
TOP = 4
SH = 2816
TOK_DEV = 128
TOKENS = 4096
SLOTS = 64
CAP = 9
N_DP = 32
N_TENSOR = 1


def draw_expert_map(key, part):
    slot_order = jax.random.permutation(jax.random.fold_in(key, 11), SLOTS)
    return slot_order[:EXPERTS].astype(jnp.int32)


def route_block(block_key):
    key_order, key_keep, key_rows, key_roll = jax.random.split(block_key, 4)
    expert_order = jax.random.permutation(key_order, EXPERTS).astype(jnp.int32)
    instance_count = EXPERTS * CAP
    row_count = TOK_DEV * TOP
    remaining = CAP + jax.random.permutation(key_keep, instance_count - CAP).astype(jnp.int32)
    keep_order = jnp.concatenate([jnp.arange(CAP, dtype=jnp.int32), remaining])
    kept_mask = jnp.zeros((instance_count,), jnp.int32).at[keep_order[:row_count]].set(1)
    kept_index = jnp.nonzero(kept_mask, size=row_count)[0].astype(jnp.int32)
    expert_named = expert_order[kept_index // CAP]
    route_grid = expert_named.reshape(TOP, TOK_DEV).T
    row_order = jax.random.permutation(key_rows, TOK_DEV).astype(jnp.int32)
    route_grid = route_grid[row_order]
    roll_by = jax.random.randint(key_roll, (TOK_DEV, 1), 0, TOP, dtype=jnp.int32)
    column_order = (jnp.arange(TOP, dtype=jnp.int32)[None, :] + roll_by) % TOP
    return jnp.take_along_axis(route_grid, column_order, axis=1).astype(jnp.int32)


def route_table(key):
    block_keys = jax.random.split(jax.random.fold_in(key, 21), TOKENS // TOK_DEV)
    return jax.vmap(route_block)(block_keys).reshape(TOKENS, TOP).astype(jnp.int32)


def expert_directions(key):
    return jnp.clip(jax.random.normal(jax.random.fold_in(key, 31), (EXPERTS, D), jnp.float32), -5.0, 5.0)


def draw_route_ids(key, part):
    return route_table(key)


def draw_tokens(key, part):
    routes = route_table(key)
    onehot = jnp.sum((routes[:, :, None] == jnp.arange(EXPERTS, dtype=jnp.int32)[None, None, :]).astype(jnp.float32), axis=1)
    lifted = jnp.dot(onehot, expert_directions(key), precision=lax.Precision.HIGHEST)
    base_noise = jnp.clip(jax.random.normal(jax.random.fold_in(key, 41), (TOKENS, D), jnp.float32), -6.0, 6.0)
    values = base_noise + 6.5 / math.sqrt(D) * lifted
    return jnp.clip(values, -8.0, 8.0).astype(jnp.bfloat16)


def draw_router(key, part):
    directions = expert_directions(key)
    spread = jnp.clip(jax.random.normal(jax.random.fold_in(key, 51), (EXPERTS, D), jnp.float32), -5.0, 5.0)
    return (jnp.transpose(directions + spread) * (0.75 / math.sqrt(D))).astype(jnp.bfloat16)


def shard_levels(own_key, extent, cuts, smallest, top_value):
    gain = 1.0
    for dim, shards_of in cuts:
        draws = jax.random.uniform(jax.random.fold_in(jax.random.fold_in(own_key, 6), dim), (shards_of,), jnp.float32, smallest / len(cuts), top_value / len(cuts))
        gain = gain * jnp.repeat(jnp.exp(draws), extent[dim] // shards_of).reshape((-1,) + (1,) * (len(extent) - 1 - dim))
    return gain


def gaussian(key, shape, scale, limit, cuts=(), kind=jnp.bfloat16):
    drawn = scale * jax.random.normal(key, shape, jnp.float32)
    if cuts:
        drawn = drawn * shard_levels(key, shape, cuts, -0.22, 0.18)
    return jnp.clip(drawn, -limit, limit).astype(kind)


def setup_inputs(seed: int = 0) -> dict:
    keys = jax.random.split(jax.random.key(seed), 13)
    tokens = draw_tokens(jax.random.fold_in(keys[12], 71), 0)
    grad_out = gaussian(keys[1], (TOKENS, D), 1.0, 6.0, ((0, 32),))
    route_ids = draw_route_ids(jax.random.fold_in(keys[12], 71), 0)
    expert_map = draw_expert_map(jax.random.fold_in(keys[12], 71), 0)
    router = draw_router(jax.random.fold_in(keys[12], 71), 0)
    shared_gate = gaussian(keys[5], (D,), D ** -0.5, 0.125)
    sh_gate = gaussian(keys[6], (D, SH), D ** -0.5, 0.125, ((0, 32),))
    sh_up = gaussian(keys[7], (D, SH), D ** -0.5, 0.125, ((0, 32),))
    sh_down = gaussian(keys[8], (SH, D), SH ** -0.5, 0.109375, ((1, 32),))
    ex_gate = gaussian(keys[9], (SLOTS, D, F), D ** -0.5, 0.125, ((0, 32),))
    ex_up = gaussian(keys[10], (SLOTS, D, F), D ** -0.5, 0.125, ((0, 32),))
    ex_down = gaussian(keys[11], (SLOTS, F, D), F ** -0.5, 0.15625, ((0, 32),))
    return dict(tokens=tokens, grad_out=grad_out, route_ids=route_ids, expert_map=expert_map, router=router, shared_gate=shared_gate, sh_gate=sh_gate, sh_up=sh_up, sh_down=sh_down, ex_gate=ex_gate, ex_up=ex_up, ex_down=ex_down)


def silu_pair(pre_gate):
    sigmoid_val = 1.0 / (1.0 + jnp.exp(-pre_gate))
    return pre_gate * sigmoid_val, sigmoid_val * (1.0 + pre_gate * (1.0 - sigmoid_val))


def contract_last(left, right):
    return lax.dot_general(left, right, (((1,), (1,)), ((), ())), preferred_element_type=jnp.float32)


def expert_block(rows_in, rows_cot, w_gate, w_up, w_down):
    pre_gate = jnp.dot(rows_in, w_gate, preferred_element_type=jnp.float32)
    pre_up = jnp.dot(rows_in, w_up, preferred_element_type=jnp.float32)
    active, derivative = silu_pair(pre_gate)
    hidden = (active * pre_up).astype(jnp.bfloat16)
    result = jnp.dot(hidden, w_down, preferred_element_type=jnp.float32)
    grad_hidden = contract_last(rows_cot, w_down)
    grad_gate = (grad_hidden * pre_up * derivative).astype(jnp.bfloat16)
    grad_up = (grad_hidden * active).astype(jnp.bfloat16)
    backward = contract_last(grad_gate, w_gate) + contract_last(grad_up, w_up)
    return result, backward


def contract_last_highest(left, right):
    return lax.dot_general(left, right, (((1,), (1,)), ((), ())), precision=lax.Precision.HIGHEST, preferred_element_type=jnp.float32)


def reference(tokens, grad_out, route_ids, expert_map, router, shared_gate, sh_gate, sh_up, sh_down, ex_gate, ex_up, ex_down):
    rows_dev = TOK_DEV * TOP
    width_part = F // N_TENSOR
    group_ids = route_ids.reshape(N_DP, rows_dev)
    chosen = (group_ids[:, :, None] == jnp.arange(EXPERTS, dtype=jnp.int32)[None, None, :]).astype(jnp.int32)
    earlier = jnp.sum((jnp.cumsum(chosen, axis=1) - chosen) * chosen, axis=2).astype(jnp.int32)
    slot_of = expert_map[group_ids].astype(jnp.int32)
    position = jnp.arange(N_DP, dtype=jnp.int32)[:, None] * CAP + earlier
    token_of = jnp.arange(N_DP * rows_dev, dtype=jnp.int32).reshape(N_DP, rows_dev) // TOP
    source = jnp.full((SLOTS, N_DP * CAP), TOKENS, jnp.int32).at[slot_of, position].set(token_of)
    zero_row = jnp.zeros((1, D), jnp.bfloat16)
    padded_in = jnp.concatenate([tokens, zero_row], axis=0)
    padded_cot = jnp.concatenate([grad_out, zero_row], axis=0)

    def run_slot(operands):
        src_rows, w_gate, w_up, w_down = operands
        rows_in = jnp.take(padded_in, src_rows, axis=0)
        rows_cot = jnp.take(padded_cot, src_rows, axis=0)
        total_out = jnp.zeros((N_DP * CAP, D), jnp.float32)
        total_back = jnp.zeros((N_DP * CAP, D), jnp.float32)
        for block_idx in range(N_TENSOR):
            low_col = block_idx * width_part
            high_col = low_col + width_part
            result, backward = expert_block(rows_in, rows_cot, w_gate[:, low_col:high_col], w_up[:, low_col:high_col], w_down[low_col:high_col, :])
            total_out = total_out + lax.optimization_barrier(result.astype(jnp.bfloat16)).astype(jnp.float32)
            total_back = total_back + lax.optimization_barrier(backward.astype(jnp.bfloat16)).astype(jnp.float32)
        return total_out, total_back

    slot_out, slot_back = lax.map(run_slot, (source, ex_gate, ex_up, ex_down))
    flat_slot = slot_of.reshape(-1)
    flat_pos = position.reshape(-1)
    expert_out = slot_out[flat_slot, flat_pos].reshape(TOKENS, TOP, D)
    expert_back = slot_back[flat_slot, flat_pos].reshape(TOKENS, TOP, D)

    logits = jnp.dot(tokens, router, preferred_element_type=jnp.float32)
    exp_logit = jnp.exp(logits)
    prob_table = exp_logit / jnp.sum(exp_logit, axis=1, keepdims=True)
    picked = (route_ids[:, :, None] == jnp.arange(EXPERTS, dtype=jnp.int32)[None, None, :]).astype(jnp.float32)
    gate_weights = jnp.sum(picked * prob_table[:, None, :], axis=2)

    sh_out, sh_back = expert_block(tokens, grad_out, sh_gate, sh_up, sh_down)
    shared_scale = 1.0 / (1.0 + jnp.exp(-jnp.dot(tokens, shared_gate, preferred_element_type=jnp.float32)))

    mixed = jnp.sum(gate_weights[:, :, None] * expert_out, axis=1) + shared_scale[:, None] * sh_out
    cot_full = grad_out.astype(jnp.float32)
    out_dots = jnp.sum(cot_full[:, None, :] * expert_out, axis=2)
    shared_dots = jnp.sum(cot_full * sh_out, axis=1)
    grad_prob = jnp.sum(picked * out_dots[:, :, None], axis=1)
    dlogits = prob_table * (grad_prob - jnp.sum(gate_weights * out_dots, axis=1, keepdims=True))
    grad_router = contract_last_highest(dlogits, router.astype(jnp.float32))
    slope_term = shared_dots * shared_scale * (1.0 - shared_scale)
    grad_total = jnp.sum(gate_weights[:, :, None] * expert_back, axis=1) + shared_scale[:, None] * sh_back
    grad_total = grad_total + grad_router + slope_term[:, None] * shared_gate.astype(jnp.float32)[None, :]
    return mixed.astype(jnp.bfloat16), grad_total.astype(jnp.bfloat16)
```

```python
import jax
import jax.numpy as jnp
from jax import lax
from jax.experimental import pallas as pl
from jax.experimental.pallas import tpu as pltpu
from jax.sharding import PartitionSpec as P

CAP = 9


def silu_pair(pre_gate):
    sigmoid_val = 1.0 / (1.0 + jnp.exp(-pre_gate))
    return (pre_gate * sigmoid_val, sigmoid_val * (1.0 + pre_gate * (1.0 - sigmoid_val)))


def contract_last(left, right):
    return lax.dot_general(
        left, right, (((1,), (1,)), ((), ())), preferred_element_type=jnp.float32
    )


def expert_block(rows_in, rows_cot, w_gate, w_up, w_down):
    pre_gate = jnp.dot(rows_in, w_gate, preferred_element_type=jnp.float32)
    pre_up = jnp.dot(rows_in, w_up, preferred_element_type=jnp.float32)
    active, derivative = silu_pair(pre_gate)
    hidden = (active * pre_up).astype(jnp.bfloat16)
    result = jnp.dot(hidden, w_down, preferred_element_type=jnp.float32)
    grad_hidden = contract_last(rows_cot, w_down)
    grad_gate = (grad_hidden * pre_up * derivative).astype(jnp.bfloat16)
    grad_up = (grad_hidden * active).astype(jnp.bfloat16)
    backward = contract_last(grad_gate, w_gate) + contract_last(grad_up, w_up)
    return (result, backward)


def expert_batch(rows_in, rows_cot, w_gate, w_up, w_down):
    pre_gate = jnp.einsum("slcd,ldf->slcf", rows_in, w_gate, preferred_element_type=jnp.float32)
    pre_up = jnp.einsum("slcd,ldf->slcf", rows_in, w_up, preferred_element_type=jnp.float32)
    active, derivative = silu_pair(pre_gate)
    hidden = (active * pre_up).astype(jnp.bfloat16)
    result = jnp.einsum(
        "slcf,lfd->slcd", hidden, w_down, preferred_element_type=jnp.float32
    ).astype(jnp.bfloat16)
    grad_hidden = jnp.einsum("slcd,lfd->slcf", rows_cot, w_down, preferred_element_type=jnp.float32)
    grad_gate = (grad_hidden * pre_up * derivative).astype(jnp.bfloat16)
    grad_up = (grad_hidden * active).astype(jnp.bfloat16)
    grad_both = jnp.concatenate([grad_gate, grad_up], axis=3)
    weight_both = jnp.concatenate([w_gate, w_up], axis=2)
    backward = jnp.einsum(
        "slcf,ldf->slcd", grad_both, weight_both, preferred_element_type=jnp.float32
    )
    return (result, backward.astype(jnp.bfloat16))


def shards(
    tokens,
    grad_out,
    route_ids,
    expert_map,
    router,
    shared_gate,
    sh_gate,
    sh_up,
    sh_down,
    ex_gate,
    ex_up,
    ex_down,
):
    tok_dev, width = tokens.shape
    top_count = route_ids.shape[1]
    expert_count = router.shape[1]
    dp_size = lax.axis_size("dp")
    tensor_size = lax.axis_size("tensor")
    tensor_rank = lax.axis_index("tensor")
    local_slots = ex_gate.shape[0]
    col_width = width // tensor_size
    col_start = tensor_rank * col_width
    buffer_rows = dp_size * local_slots * CAP
    slot_rows = local_slots * CAP
    flat_ids = route_ids.reshape(-1)
    chosen = (flat_ids[:, None] == jnp.arange(expert_count, dtype=jnp.int32)[None, :]).astype(
        jnp.int32
    )
    earlier = jnp.sum((jnp.cumsum(chosen, axis=0) - chosen) * chosen, axis=1)
    slot_of = jnp.sum(chosen * expert_map[None, :], axis=1)
    position = slot_of * CAP + earlier
    token_index = jnp.arange(tok_dev * top_count, dtype=jnp.int32) // top_count
    source_rows = jnp.full((buffer_rows,), tok_dev, jnp.int32).at[position].set(token_index)

    def fetch_rows(table):
        padded = jnp.concatenate([table, jnp.zeros((1, table.shape[1]), table.dtype)], axis=0)
        return jnp.take(padded, source_rows, axis=0)

    send_in = fetch_rows(tokens).reshape(dp_size, slot_rows, width)
    send_cot = fetch_rows(grad_out).reshape(dp_size, slot_rows, width)
    got_in = lax.all_to_all(send_in, "dp", split_axis=0, concat_axis=0, tiled=True)
    got_cot = lax.all_to_all(send_cot, "dp", split_axis=0, concat_axis=0, tiled=True)
    grid_shape = (dp_size, local_slots, CAP, width)
    result, backward = expert_batch(
        got_in.reshape(grid_shape), got_cot.reshape(grid_shape), ex_gate, ex_up, ex_down
    )
    came_out = lax.all_to_all(
        result.reshape(dp_size, slot_rows, width), "dp", split_axis=0, concat_axis=0, tiled=True
    )
    came_back = lax.all_to_all(
        backward.reshape(dp_size, slot_rows, width), "dp", split_axis=0, concat_axis=0, tiled=True
    )
    routed_out = came_out.reshape(buffer_rows, width)
    routed_back = came_back.reshape(buffer_rows, width)
    weights = (
        lax.all_gather(sh_gate, "dp", axis=0, tiled=True),
        lax.all_gather(sh_up, "dp", axis=0, tiled=True),
        lax.all_gather(sh_down, "dp", axis=1, tiled=True),
    )
    full_gate, full_up, full_down = weights
    sh_out, sh_back = expert_block(tokens, grad_out, full_gate, full_up, full_down)
    routed_width = routed_out.shape[1]
    expert_out = jnp.take(routed_out, position, axis=0).reshape(tok_dev, top_count, routed_width)
    expert_back = jnp.take(routed_back, position, axis=0).reshape(tok_dev, top_count, routed_width)
    logits = jnp.dot(tokens, router, preferred_element_type=jnp.float32)
    exp_logit = jnp.exp(logits)
    prob_table = exp_logit / jnp.sum(exp_logit, axis=1, keepdims=True)
    picked = chosen.reshape(tok_dev, top_count, expert_count).astype(jnp.float32)
    gate_weights = jnp.sum(picked * prob_table[:, None, :], axis=2)
    shared_scale = 1.0 / (
        1.0 + jnp.exp(-jnp.dot(tokens, shared_gate, preferred_element_type=jnp.float32))
    )
    shared_part = jnp.sum(grad_out.astype(jnp.float32) * sh_out, axis=1)
    dots_part = jnp.einsum("td,tkd->tk", grad_out, expert_out, preferred_element_type=jnp.float32)
    mixed_part = (
        jnp.sum(gate_weights[:, :, None] * expert_out.astype(jnp.float32), axis=1)
        + shared_scale[:, None] * sh_out
    )
    grad_part = (
        jnp.sum(gate_weights[:, :, None] * expert_back.astype(jnp.float32), axis=1)
        + shared_scale[:, None] * sh_back
    )
    out_dots, shared_dots = lax.psum((dots_part, shared_part), "tensor")
    mixed_cols, grad_cols = (
        lax.psum_scatter(mixed_part, "tensor", scatter_dimension=1, tiled=True),
        lax.psum_scatter(grad_part, "tensor", scatter_dimension=1, tiled=True),
    )
    grad_prob = jnp.sum(picked * out_dots[:, :, None], axis=1)
    dlogits = prob_table * (grad_prob - jnp.sum(gate_weights * out_dots, axis=1, keepdims=True))
    router_cols = lax.dynamic_slice_in_dim(router, col_start, col_width, 0).astype(jnp.float32)
    grad_router = lax.dot_general(
        dlogits,
        router_cols,
        (((1,), (1,)), ((), ())),
        precision=lax.Precision.HIGHEST,
        preferred_element_type=jnp.float32,
    )
    gate_cols = lax.dynamic_slice_in_dim(shared_gate, col_start, col_width, 0).astype(jnp.float32)
    slope_term = shared_dots * shared_scale * (1.0 - shared_scale)
    grad_total = grad_cols + grad_router + slope_term[:, None] * gate_cols[None, :]
    return (mixed_cols.astype(jnp.bfloat16), grad_total.astype(jnp.bfloat16))


def dot32(left, right):
    return jnp.dot(left, right, preferred_element_type=jnp.float32)


def expert_hidden(rows_in, w_gate, w_up):
    pre_gate = jnp.einsum("slcd,ldf->slcf", rows_in, w_gate, preferred_element_type=jnp.float32)
    pre_up = jnp.einsum("slcd,ldf->slcf", rows_in, w_up, preferred_element_type=jnp.float32)
    return pre_gate, pre_up


def reorder_kernel(order_ref, *refs):
    count = len(refs) // 2
    for source, target in zip(refs[:count], refs[count:]):
        target[...] = source[...]


def reorder_blocks(order, stacks):
    blocks, rows, cols = stacks[0].shape
    spec_in = pl.BlockSpec((1, rows, cols), lambda j, order_ref: (order_ref[j], 0, 0))
    spec_out = pl.BlockSpec((1, rows, cols), lambda j, order_ref: (j, 0, 0))
    size = sum(s.size * s.dtype.itemsize for s in stacks)
    return pl.pallas_call(
        reorder_kernel,
        grid_spec=pltpu.PrefetchScalarGridSpec(
            num_scalar_prefetch=1,
            grid=(blocks,),
            in_specs=[spec_in] * len(stacks),
            out_specs=[spec_out] * len(stacks),
        ),
        out_shape=[jax.ShapeDtypeStruct(s.shape, s.dtype) for s in stacks],
        cost_estimate=pl.CostEstimate(
            flops=4 * size, bytes_accessed=2 * size, transcendentals=0
        ),
    )(order, *stacks)


def paired_shards(
    tokens,
    grad_out,
    route_ids,
    expert_map,
    router,
    shared_gate,
    sh_gate,
    sh_up,
    sh_down,
    ex_gate,
    ex_up,
    ex_down,
):
    tok_dev, width = tokens.shape
    top_count = route_ids.shape[1]
    expert_count = router.shape[1]
    dp_size = lax.axis_size("dp")
    local_slots = ex_gate.shape[0]
    half_size = dp_size // 2
    lanes = half_size // 2
    lane_bits = lanes.bit_length() - 1
    rows_slot = -(-4 * CAP // 8) * 8
    rows_all = lanes * local_slots * rows_slot
    me = lax.axis_index("dp")
    half = me // half_size
    lane = (me % half_size) // 2
    core = me % 2
    pair_half = [(i, i ^ half_size) for i in range(dp_size)]
    pair_core = [(i, i ^ 1) for i in range(dp_size)]
    lane_groups = [
        [h * half_size + 2 * n + c for n in range(lanes)] for h in range(2) for c in range(2)
    ]

    def across(value, pairs):
        return lax.ppermute(value, "dp", pairs)

    def exchange(value):
        return lax.all_to_all(
            value, "dp", split_axis=0, concat_axis=0, tiled=True, axis_index_groups=lane_groups
        )

    tokens_two = jnp.concatenate([tokens, across(tokens, pair_half)], axis=0)
    grads_two = jnp.concatenate([grad_out, across(grad_out, pair_half)], axis=0)

    chosen = (
        route_ids[:, :, None] == jnp.arange(expert_count, dtype=jnp.int32)[None, None, :]
    ).astype(jnp.float32)
    named = jnp.sum(chosen, axis=1)
    before = (
        jnp.arange(tok_dev, dtype=jnp.int32)[:, None]
        > jnp.arange(tok_dev, dtype=jnp.int32)[None, :]
    ).astype(jnp.bfloat16)
    earlier = dot32(before, named.astype(jnp.bfloat16))
    rank = jnp.sum(chosen * earlier[:, None, :], axis=2)
    slot = jnp.sum(chosen * expert_map.astype(jnp.float32)[None, None, :], axis=2)
    logits = dot32(tokens, router)
    exp_logit = jnp.exp(logits)
    prob_table = exp_logit / jnp.sum(exp_logit, axis=1, keepdims=True)
    gate_weights = jnp.sum(chosen * prob_table[:, None, :], axis=2)
    shared_scale = 1.0 / (1.0 + jnp.exp(-dot32(tokens, shared_gate)))
    meta = jnp.concatenate([slot, rank, gate_weights, shared_scale[:, None]], axis=1)
    meta_two = jnp.concatenate([meta, across(meta, pair_half)], axis=0)
    meta_all = jnp.concatenate([meta_two, across(meta_two, pair_core)], axis=0)
    tokens_all = jnp.concatenate([tokens_two, across(tokens_two, pair_core)], axis=0)
    grads_all = jnp.concatenate([grads_two, across(grads_two, pair_core)], axis=0)
    tok_all = 4 * tok_dev

    slot_all = meta_all[:, :top_count].astype(jnp.int32)
    rank_all = meta_all[:, top_count : 2 * top_count].astype(jnp.int32)
    gates_all = meta_all[:, 2 * top_count : 3 * top_count]
    scale_all = meta_all[:, 3 * top_count :]
    holder = slot_all // local_slots
    block = jnp.arange(tok_all, dtype=jnp.int32)[:, None] // tok_dev
    row_at = ((holder % half_size) // 2) * local_slots + slot_all % local_slots
    row_at = row_at * rows_slot + block * CAP + rank_all
    row_at = jnp.where((holder // half_size == half) & (holder % 2 == core), row_at, -1)
    row_ids = jnp.arange(rows_all, dtype=jnp.int32)
    pick_rows = jnp.sum(
        (row_at.T[:, None, :] == row_ids[None, :, None]).astype(jnp.float32), axis=0
    ).astype(jnp.bfloat16)
    hit = row_at[:, :, None] == row_ids[None, None, :]
    place = jnp.sum(jnp.where(hit, gates_all[:, :, None], 0.0), axis=1).astype(jnp.bfloat16)

    def dispatch(table):
        rows = dot32(pick_rows, table).astype(jnp.bfloat16)
        got = exchange(rows.reshape(lanes, local_slots * rows_slot, width))
        return got.reshape(lanes, local_slots, rows_slot, width)

    def give_back(rows):
        sent = rows.reshape(lanes, local_slots * rows_slot, width)
        return exchange(sent).reshape(rows_all, width)

    got_in = dispatch(tokens_all)
    got_cot = dispatch(grads_all)

    hidden_all = sh_gate.shape[1]
    quarter = hidden_all // 4
    quarter_pad = -(-quarter // 128) * 128
    shard = jnp.stack([sh_gate, sh_up, sh_down.T]).reshape(3, width // dp_size, 4, quarter)
    shard = jnp.pad(shard, ((0, 0), (0, 0), (0, 0), (0, quarter_pad - quarter)))
    shard = shard.transpose(2, 0, 1, 3).reshape(2, 2, 3, width // dp_size, quarter_pad)
    kept = lax.dynamic_index_in_dim(shard, core, 0, keepdims=False)
    came = across(lax.dynamic_index_in_dim(shard, 1 - core, 0, keepdims=False), pair_core)
    both = jnp.where(
        core == 0, jnp.concatenate([kept, came], axis=2), jnp.concatenate([came, kept], axis=2)
    )
    own_rows = lax.dynamic_index_in_dim(both, half, 0, keepdims=False)
    far_rows = across(lax.dynamic_index_in_dim(both, 1 - half, 0, keepdims=False), pair_half)

    def spread(piece, first_bit):
        held = piece[None]
        bits = [(first_bit + s) % lane_bits for s in range(lane_bits)]
        for bit in bits:
            pairs = [(i, i ^ (2 << bit)) for i in range(dp_size)]
            held = jnp.concatenate([held, across(held, pairs)], axis=0)
        place_of = {}
        for index in range(lanes):
            place_of[sum(((index >> s) & 1) << bit for s, bit in enumerate(bits))] = index
        return [held[place_of[d] : place_of[d] + 1] for d in range(lanes)]

    pieces = [[spread(part[w], w % lane_bits) for part in (own_rows, far_rows)] for w in range(3)]
    stacks = [jnp.concatenate(p[0] + p[1], axis=0) for p in pieces]
    index = jnp.arange(2 * lanes, dtype=jnp.int32)
    order = ((index // lanes) ^ half) * lanes + ((index % lanes) ^ lane)
    full_gate, full_up, full_down = [
        s.reshape(width, quarter_pad) for s in reorder_blocks(order, stacks)
    ]

    pre_gate, pre_up = expert_hidden(got_in, ex_gate, ex_up)
    active, derivative = silu_pair(pre_gate)
    hidden = (active * pre_up).astype(jnp.bfloat16)
    result = jnp.einsum(
        "slcf,lfd->slcd", hidden, ex_down, preferred_element_type=jnp.float32
    ).astype(jnp.bfloat16)
    routed_out = give_back(result)
    grad_hidden = jnp.einsum("slcd,lfd->slcf", got_cot, ex_down, preferred_element_type=jnp.float32)
    grad_gate = (grad_hidden * pre_up * derivative).astype(jnp.bfloat16)
    grad_up = (grad_hidden * active).astype(jnp.bfloat16)
    grad_both = jnp.concatenate([grad_gate, grad_up], axis=3)
    weight_both = jnp.concatenate([ex_gate, ex_up], axis=2)
    backward = jnp.einsum(
        "slcf,ldf->slcd", grad_both, weight_both, preferred_element_type=jnp.float32
    )
    routed_back = give_back(backward.astype(jnp.bfloat16))

    sh_pre_gate = dot32(tokens_all, full_gate)
    sh_pre_up = dot32(tokens_all, full_up)
    sh_active, sh_derivative = silu_pair(sh_pre_gate)
    sh_hidden = (sh_active * sh_pre_up).astype(jnp.bfloat16)
    sh_out = contract_last(sh_hidden, full_down)
    sh_grad_hidden = dot32(grads_all, full_down)
    sh_grad_gate = (sh_grad_hidden * sh_pre_up * sh_derivative).astype(jnp.bfloat16)
    sh_grad_up = (sh_grad_hidden * sh_active).astype(jnp.bfloat16)
    sh_back = contract_last(sh_grad_gate, full_gate) + contract_last(sh_grad_up, full_up)

    def collect(partial):
        here = partial[: 2 * tok_dev]
        pair_sum = here + across(partial[2 * tok_dev :].astype(jnp.bfloat16), pair_core).astype(
            jnp.float32
        )
        return pair_sum[:tok_dev] + across(
            pair_sum[tok_dev:].astype(jnp.bfloat16), pair_half
        ).astype(jnp.float32)

    mixed = collect(dot32(place, routed_out) + scale_all * sh_out)
    all_dots = contract_last(grads_all, routed_out)
    dots_part = jnp.sum(jnp.where(hit, all_dots[:, None, :], 0.0), axis=2)
    shared_part = jnp.sum(grads_all.astype(jnp.float32) * sh_out, axis=1, keepdims=True)
    scalars = jnp.concatenate([dots_part, shared_part], axis=1)
    scalars = scalars[: 2 * tok_dev] + across(scalars[2 * tok_dev :], pair_core)
    scalars = scalars[:tok_dev] + across(scalars[tok_dev:], pair_half)
    out_dots = scalars[:, :top_count]
    shared_dots = scalars[:, top_count]
    grad_part = collect(dot32(place, routed_back) + scale_all * sh_back)

    grad_prob = jnp.sum(chosen * out_dots[:, :, None], axis=1)
    dlogits = prob_table * (grad_prob - jnp.sum(gate_weights * out_dots, axis=1, keepdims=True))
    grad_router = lax.dot_general(
        dlogits,
        router.astype(jnp.float32),
        (((1,), (1,)), ((), ())),
        precision=lax.Precision.HIGHEST,
        preferred_element_type=jnp.float32,
    )
    slope_term = shared_dots * shared_scale * (1.0 - shared_scale)
    grad_total = (
        grad_part + grad_router + slope_term[:, None] * shared_gate.astype(jnp.float32)[None, :]
    )
    return (mixed.astype(jnp.bfloat16), grad_total.astype(jnp.bfloat16))


def solution(mesh):
    dp_size = mesh.shape["dp"]
    paired = mesh.shape["tensor"] == 1 and dp_size >= 8 and dp_size & (dp_size - 1) == 0
    placed = (
        P("dp", None),
        P("dp", None),
        P("dp", None),
        P(),
        P(),
        P(),
        P("dp", "tensor"),
        P("dp", "tensor"),
        P("tensor", "dp"),
        P("dp", None, "tensor"),
        P("dp", None, "tensor"),
        P("dp", "tensor", None),
    )
    return jax.shard_map(
        paired_shards if paired else shards,
        mesh=mesh,
        in_specs=placed,
        out_specs=(P("dp", "tensor"), P("dp", "tensor")),
        check_vma=False,
    )
```

```python
import jax
import jax.numpy as jnp
from jax import lax
from jax.experimental import pallas as pl
from jax.experimental.pallas import tpu as pltpu
from jax.sharding import PartitionSpec as P


CAP = 9


def silu_pair(pre_gate):
    sigmoid_val = 1.0 / (1.0 + jnp.exp(-pre_gate))
    return (pre_gate * sigmoid_val, sigmoid_val * (1.0 + pre_gate * (1.0 - sigmoid_val)))


def contract_last(left, right):
    return lax.dot_general(
        left, right, (((1,), (1,)), ((), ())), preferred_element_type=jnp.float32
    )


def expert_block(rows_in, rows_cot, w_gate, w_up, w_down):
    pre_gate = jnp.dot(rows_in, w_gate, preferred_element_type=jnp.float32)
    pre_up = jnp.dot(rows_in, w_up, preferred_element_type=jnp.float32)
    active, derivative = silu_pair(pre_gate)
    hidden = (active * pre_up).astype(jnp.bfloat16)
    result = jnp.dot(hidden, w_down, preferred_element_type=jnp.float32)
    grad_hidden = contract_last(rows_cot, w_down)
    grad_gate = (grad_hidden * pre_up * derivative).astype(jnp.bfloat16)
    grad_up = (grad_hidden * active).astype(jnp.bfloat16)
    backward = contract_last(grad_gate, w_gate) + contract_last(grad_up, w_up)
    return (result, backward)


def expert_batch(rows_in, rows_cot, w_gate, w_up, w_down):
    pre_gate = jnp.einsum("slcd,ldf->slcf", rows_in, w_gate, preferred_element_type=jnp.float32)
    pre_up = jnp.einsum("slcd,ldf->slcf", rows_in, w_up, preferred_element_type=jnp.float32)
    active, derivative = silu_pair(pre_gate)
    hidden = (active * pre_up).astype(jnp.bfloat16)
    result = jnp.einsum(
        "slcf,lfd->slcd", hidden, w_down, preferred_element_type=jnp.float32
    ).astype(jnp.bfloat16)
    grad_hidden = jnp.einsum("slcd,lfd->slcf", rows_cot, w_down, preferred_element_type=jnp.float32)
    grad_gate = (grad_hidden * pre_up * derivative).astype(jnp.bfloat16)
    grad_up = (grad_hidden * active).astype(jnp.bfloat16)
    grad_both = jnp.concatenate([grad_gate, grad_up], axis=3)
    weight_both = jnp.concatenate([w_gate, w_up], axis=2)
    backward = jnp.einsum(
        "slcf,ldf->slcd", grad_both, weight_both, preferred_element_type=jnp.float32
    )
    return (result, backward.astype(jnp.bfloat16))


def shards(
    tokens,
    grad_out,
    route_ids,
    expert_map,
    router,
    shared_gate,
    sh_gate,
    sh_up,
    sh_down,
    ex_gate,
    ex_up,
    ex_down,
):
    tok_dev, width = tokens.shape
    top_count = route_ids.shape[1]
    expert_count = router.shape[1]
    dp_size = lax.axis_size("dp")
    tensor_size = lax.axis_size("tensor")
    tensor_rank = lax.axis_index("tensor")
    local_slots = ex_gate.shape[0]
    col_width = width // tensor_size
    col_start = tensor_rank * col_width
    buffer_rows = dp_size * local_slots * CAP
    slot_rows = local_slots * CAP
    flat_ids = route_ids.reshape(-1)
    chosen = (flat_ids[:, None] == jnp.arange(expert_count, dtype=jnp.int32)[None, :]).astype(
        jnp.int32
    )
    earlier = jnp.sum((jnp.cumsum(chosen, axis=0) - chosen) * chosen, axis=1)
    slot_of = jnp.sum(chosen * expert_map[None, :], axis=1)
    position = slot_of * CAP + earlier
    token_index = jnp.arange(tok_dev * top_count, dtype=jnp.int32) // top_count
    source_rows = jnp.full((buffer_rows,), tok_dev, jnp.int32).at[position].set(token_index)

    def fetch_rows(table):
        padded = jnp.concatenate([table, jnp.zeros((1, table.shape[1]), table.dtype)], axis=0)
        return jnp.take(padded, source_rows, axis=0)

    send_in = fetch_rows(tokens).reshape(dp_size, slot_rows, width)
    send_cot = fetch_rows(grad_out).reshape(dp_size, slot_rows, width)
    got_in = lax.all_to_all(send_in, "dp", split_axis=0, concat_axis=0, tiled=True)
    got_cot = lax.all_to_all(send_cot, "dp", split_axis=0, concat_axis=0, tiled=True)
    grid_shape = (dp_size, local_slots, CAP, width)
    result, backward = expert_batch(
        got_in.reshape(grid_shape), got_cot.reshape(grid_shape), ex_gate, ex_up, ex_down
    )
    came_out = lax.all_to_all(
        result.reshape(dp_size, slot_rows, width), "dp", split_axis=0, concat_axis=0, tiled=True
    )
    came_back = lax.all_to_all(
        backward.reshape(dp_size, slot_rows, width), "dp", split_axis=0, concat_axis=0, tiled=True
    )
    routed_out = came_out.reshape(buffer_rows, width)
    routed_back = came_back.reshape(buffer_rows, width)
    weights = (
        lax.all_gather(sh_gate, "dp", axis=0, tiled=True),
        lax.all_gather(sh_up, "dp", axis=0, tiled=True),
        lax.all_gather(sh_down, "dp", axis=1, tiled=True),
    )
    full_gate, full_up, full_down = weights
    sh_out, sh_back = expert_block(tokens, grad_out, full_gate, full_up, full_down)
    routed_width = routed_out.shape[1]
    expert_out = jnp.take(routed_out, position, axis=0).reshape(tok_dev, top_count, routed_width)
    expert_back = jnp.take(routed_back, position, axis=0).reshape(tok_dev, top_count, routed_width)
    logits = jnp.dot(tokens, router, preferred_element_type=jnp.float32)
    exp_logit = jnp.exp(logits)
    prob_table = exp_logit / jnp.sum(exp_logit, axis=1, keepdims=True)
    picked = chosen.reshape(tok_dev, top_count, expert_count).astype(jnp.float32)
    gate_weights = jnp.sum(picked * prob_table[:, None, :], axis=2)
    shared_scale = 1.0 / (
        1.0 + jnp.exp(-jnp.dot(tokens, shared_gate, preferred_element_type=jnp.float32))
    )
    shared_part = jnp.sum(grad_out.astype(jnp.float32) * sh_out, axis=1)
    dots_part = jnp.einsum("td,tkd->tk", grad_out, expert_out, preferred_element_type=jnp.float32)
    mixed_part = (
        jnp.sum(gate_weights[:, :, None] * expert_out.astype(jnp.float32), axis=1)
        + shared_scale[:, None] * sh_out
    )
    grad_part = (
        jnp.sum(gate_weights[:, :, None] * expert_back.astype(jnp.float32), axis=1)
        + shared_scale[:, None] * sh_back
    )
    out_dots, shared_dots = lax.psum((dots_part, shared_part), "tensor")
    mixed_cols, grad_cols = (
        lax.psum_scatter(mixed_part, "tensor", scatter_dimension=1, tiled=True),
        lax.psum_scatter(grad_part, "tensor", scatter_dimension=1, tiled=True),
    )
    grad_prob = jnp.sum(picked * out_dots[:, :, None], axis=1)
    dlogits = prob_table * (grad_prob - jnp.sum(gate_weights * out_dots, axis=1, keepdims=True))
    router_cols = lax.dynamic_slice_in_dim(router, col_start, col_width, 0).astype(jnp.float32)
    grad_router = lax.dot_general(
        dlogits,
        router_cols,
        (((1,), (1,)), ((), ())),
        precision=lax.Precision.HIGHEST,
        preferred_element_type=jnp.float32,
    )
    gate_cols = lax.dynamic_slice_in_dim(shared_gate, col_start, col_width, 0).astype(jnp.float32)
    slope_term = shared_dots * shared_scale * (1.0 - shared_scale)
    grad_total = grad_cols + grad_router + slope_term[:, None] * gate_cols[None, :]
    return (mixed_cols.astype(jnp.bfloat16), grad_total.astype(jnp.bfloat16))


def dot32(left, right):
    return jnp.dot(left, right, preferred_element_type=jnp.float32)


def expert_hidden(rows_in, w_gate, w_up):
    pre_gate = jnp.einsum("slcd,ldf->slcf", rows_in, w_gate, preferred_element_type=jnp.float32)
    pre_up = jnp.einsum("slcd,ldf->slcf", rows_in, w_up, preferred_element_type=jnp.float32)
    return pre_gate, pre_up


def assemble_kernel(order_ref, stacks, targets):
    first = 0
    for source, low in stacks:
        blocks, _, rows, _ = source.shape
        for j in range(blocks):
            for w, target in enumerate(targets):
                target[order_ref[first + j], low : low + rows, :] = source[j, w]
        first += blocks


def assemble(order, stacks, lows, shape):
    def kernel(order_ref, *refs):
        assemble_kernel(order_ref, list(zip(refs[:-3], lows)), refs[-3:])

    size = 3 * 2 * shape[0] * shape[1] * shape[2]
    return pl.pallas_call(
        kernel,
        in_specs=[pl.BlockSpec(memory_space=pltpu.SMEM)]
        + [pl.BlockSpec(memory_space=pltpu.VMEM)] * len(stacks),
        out_specs=[pl.BlockSpec(memory_space=pltpu.VMEM)] * 3,
        out_shape=[jax.ShapeDtypeStruct(shape, stacks[0].dtype)] * 3,
        cost_estimate=pl.CostEstimate(
            flops=100 * size, bytes_accessed=2 * size, transcendentals=0
        ),
    )(order, *stacks)


def after(value, *others):
    return lax.optimization_barrier((value,) + others)[0]


def paired_shards(
    tokens,
    grad_out,
    route_ids,
    expert_map,
    router,
    shared_gate,
    sh_gate,
    sh_up,
    sh_down,
    ex_gate,
    ex_up,
    ex_down,
):
    tok_dev, width = tokens.shape
    top_count = route_ids.shape[1]
    expert_count = router.shape[1]
    dp_size = lax.axis_size("dp")
    local_slots = ex_gate.shape[0]
    half_size = dp_size // 2
    lanes = half_size // 2
    lane_bits = lanes.bit_length() - 1
    rows_slot = -(-4 * CAP // 8) * 8
    rows_all = lanes * local_slots * rows_slot
    me = lax.axis_index("dp")
    half = me // half_size
    lane = (me % half_size) // 2
    core = me % 2
    pair_half = [(i, i ^ half_size) for i in range(dp_size)]
    pair_core = [(i, i ^ 1) for i in range(dp_size)]
    lane_groups = [
        [h * half_size + 2 * n + c for n in range(lanes)] for h in range(2) for c in range(2)
    ]

    def across(value, pairs):
        return lax.ppermute(value, "dp", pairs)

    def exchange(value):
        return lax.all_to_all(
            value, "dp", split_axis=0, concat_axis=0, tiled=True, axis_index_groups=lane_groups
        )

    tokens_far = across(tokens, pair_half)
    grads_far = across(after(grad_out, tokens_far), pair_half)
    tokens_two = jnp.concatenate([tokens, tokens_far], axis=0)
    grads_two = jnp.concatenate([grad_out, grads_far], axis=0)

    chosen = (
        route_ids[:, :, None] == jnp.arange(expert_count, dtype=jnp.int32)[None, None, :]
    ).astype(jnp.float32)
    named = jnp.sum(chosen, axis=1)
    before = (
        jnp.arange(tok_dev, dtype=jnp.int32)[:, None]
        > jnp.arange(tok_dev, dtype=jnp.int32)[None, :]
    ).astype(jnp.bfloat16)
    earlier = dot32(before, named.astype(jnp.bfloat16))
    rank = jnp.sum(chosen * earlier[:, None, :], axis=2)
    slot = jnp.sum(chosen * expert_map.astype(jnp.float32)[None, None, :], axis=2)
    logits = dot32(tokens, router)
    exp_logit = jnp.exp(logits)
    prob_table = exp_logit / jnp.sum(exp_logit, axis=1, keepdims=True)
    gate_weights = jnp.sum(chosen * prob_table[:, None, :], axis=2)
    shared_scale = 1.0 / (1.0 + jnp.exp(-dot32(tokens, shared_gate)))
    meta = jnp.concatenate([slot, rank, gate_weights, shared_scale[:, None]], axis=1)
    meta_two = jnp.concatenate([meta, across(meta, pair_half)], axis=0)
    meta_all = jnp.concatenate([meta_two, across(meta_two, pair_core)], axis=0)
    tokens_all = jnp.concatenate([tokens_two, across(tokens_two, pair_core)], axis=0)
    grads_all = jnp.concatenate([grads_two, across(grads_two, pair_core)], axis=0)
    tok_all = 4 * tok_dev

    slot_all = meta_all[:, :top_count].astype(jnp.int32)
    rank_all = meta_all[:, top_count : 2 * top_count].astype(jnp.int32)
    gates_all = meta_all[:, 2 * top_count : 3 * top_count]
    scale_all = meta_all[:, 3 * top_count :]
    holder = slot_all // local_slots
    block = jnp.arange(tok_all, dtype=jnp.int32)[:, None] // tok_dev
    row_at = ((holder % half_size) // 2) * local_slots + slot_all % local_slots
    row_at = row_at * rows_slot + block * CAP + rank_all
    row_at = jnp.where((holder // half_size == half) & (holder % 2 == core), row_at, -1)
    row_ids = jnp.arange(rows_all, dtype=jnp.int32)
    pick_rows = jnp.sum(
        (row_at.T[:, None, :] == row_ids[None, :, None]).astype(jnp.float32), axis=0
    ).astype(jnp.bfloat16)
    hit = row_at[:, :, None] == row_ids[None, None, :]
    place = jnp.sum(jnp.where(hit, gates_all[:, :, None], 0.0), axis=1).astype(jnp.bfloat16)

    def dispatch(table):
        rows = dot32(pick_rows, table).astype(jnp.bfloat16)
        got = exchange(rows.reshape(lanes, local_slots * rows_slot, width))
        return got.reshape(lanes, local_slots, rows_slot, width)

    def give_back(rows):
        sent = rows.reshape(lanes, local_slots * rows_slot, width)
        return exchange(sent).reshape(rows_all, width)

    got_in = dispatch(tokens_all)
    got_cot = dispatch(grads_all)

    hidden_all = sh_gate.shape[1]
    quarter = hidden_all // 4
    quarter_pad = -(-quarter // 128) * 128
    shard = jnp.stack([sh_gate, sh_up, sh_down.T]).reshape(3, width // dp_size, 4, quarter)
    shard = jnp.pad(shard, ((0, 0), (0, 0), (0, 0), (0, quarter_pad - quarter)))
    shard = shard.transpose(2, 0, 1, 3).reshape(2, 2, 3, width // dp_size, quarter_pad)
    kept = lax.dynamic_index_in_dim(shard, core, 0, keepdims=False)
    sent = lax.dynamic_index_in_dim(shard, 1 - core, 0, keepdims=False)
    came = across(sent, pair_core)
    both = jnp.where(
        core == 0, jnp.concatenate([kept, came], axis=2), jnp.concatenate([came, kept], axis=2)
    )
    own_rows = lax.dynamic_index_in_dim(both, half, 0, keepdims=False)
    far_rows = lax.dynamic_index_in_dim(both, 1 - half, 0, keepdims=False)
    far_rows = across(after(far_rows, grads_far), pair_half)

    def lane_hop(value, bit):
        return across(value, [(i, i ^ (2 * bit)) for i in range(dp_size)])

    def spread(block):
        top = lanes // 2
        held_all = jnp.stack([block, lane_hop(block, top)])
        chains = max(lane_bits - 1, 1)
        rows = block.shape[1] // chains
        stacks, lows, sources = [], [], []
        for chain in range(chains):
            held, came_from = held_all[:, :, chain * rows : (chain + 1) * rows], [0, top]
            bits = [1 << ((chain + step) % chains) for step in range(lane_bits - 1)]
            for step, bit in enumerate(bits):
                received = lane_hop(held, bit)
                moved = [d ^ bit for d in came_from]
                if step == len(bits) - 1:
                    stacks += [held, received]
                    lows += [chain * rows] * 2
                    sources += came_from + moved
                else:
                    held = jnp.concatenate([held, received], axis=0)
                    came_from = came_from + moved
        return stacks, lows, sources

    pre_gate, pre_up = expert_hidden(got_in, ex_gate, ex_up)
    active, derivative = silu_pair(pre_gate)
    hidden = (active * pre_up).astype(jnp.bfloat16)
    result = jnp.einsum(
        "slcf,lfd->slcd", hidden, ex_down, preferred_element_type=jnp.float32
    ).astype(jnp.bfloat16)
    routed_out = give_back(result)
    grad_hidden = jnp.einsum("slcd,lfd->slcf", got_cot, ex_down, preferred_element_type=jnp.float32)
    grad_gate = (grad_hidden * pre_up * derivative).astype(jnp.bfloat16)
    grad_up = (grad_hidden * active).astype(jnp.bfloat16)
    grad_both = jnp.concatenate([grad_gate, grad_up], axis=3)
    weight_both = jnp.concatenate([ex_gate, ex_up], axis=2)
    backward = jnp.einsum(
        "slcf,ldf->slcd", grad_both, weight_both, preferred_element_type=jnp.float32
    ).astype(jnp.bfloat16)
    routed_back = give_back(backward)

    own_stacks, own_lows, sources = spread(own_rows)
    far_stacks, far_lows, _ = spread(far_rows)
    lanes_of = jnp.array(sources, jnp.int32) ^ lane
    order = jnp.concatenate([half * lanes + lanes_of, (1 - half) * lanes + lanes_of])
    full = assemble(
        order,
        own_stacks + far_stacks,
        own_lows + far_lows,
        (2 * lanes, own_rows.shape[1], quarter_pad),
    )
    full_gate, full_up, full_down = [f.reshape(width, quarter_pad) for f in full]

    sh_pre_gate = dot32(tokens_all, full_gate)
    sh_pre_up = dot32(tokens_all, full_up)
    sh_active, sh_derivative = silu_pair(sh_pre_gate)
    sh_hidden = (sh_active * sh_pre_up).astype(jnp.bfloat16)
    sh_out = contract_last(sh_hidden, full_down)
    mixed_part = dot32(place, routed_out) + scale_all * sh_out
    sh_grad_hidden = dot32(grads_all, full_down)
    sh_grad_gate = (sh_grad_hidden * sh_pre_up * sh_derivative).astype(jnp.bfloat16)
    sh_grad_up = (sh_grad_hidden * sh_active).astype(jnp.bfloat16)
    sh_back = contract_last(sh_grad_gate, full_gate) + contract_last(sh_grad_up, full_up)
    sh_back = lax.optimization_barrier(scale_all * sh_back)

    def collect(partial):
        sent = partial[2 * tok_dev :].astype(jnp.bfloat16)
        came = across(sent, pair_core).astype(jnp.float32)
        pair_sum = partial[: 2 * tok_dev] + came
        sent = pair_sum[tok_dev:].astype(jnp.bfloat16)
        return pair_sum[:tok_dev] + across(sent, pair_half).astype(jnp.float32)

    mixed = collect(mixed_part)
    all_dots = contract_last(grads_all, routed_out)
    dots_part = jnp.sum(jnp.where(hit, all_dots[:, None, :], 0.0), axis=2)
    shared_part = jnp.sum(grads_all.astype(jnp.float32) * sh_out, axis=1, keepdims=True)
    scalars = jnp.concatenate([dots_part, shared_part], axis=1)
    scalars = scalars[: 2 * tok_dev] + across(scalars[2 * tok_dev :], pair_core)
    scalars = scalars[:tok_dev] + across(scalars[tok_dev:], pair_half)
    out_dots = scalars[:, :top_count]
    shared_dots = scalars[:, top_count]
    grad_part = collect(dot32(place, routed_back) + sh_back)

    grad_prob = jnp.sum(chosen * out_dots[:, :, None], axis=1)
    dlogits = prob_table * (grad_prob - jnp.sum(gate_weights * out_dots, axis=1, keepdims=True))
    grad_router = lax.dot_general(
        dlogits,
        router.astype(jnp.float32),
        (((1,), (1,)), ((), ())),
        precision=lax.Precision.HIGHEST,
        preferred_element_type=jnp.float32,
    )
    slope_term = shared_dots * shared_scale * (1.0 - shared_scale)
    grad_total = (
        grad_part + grad_router + slope_term[:, None] * shared_gate.astype(jnp.float32)[None, :]
    )
    return (mixed.astype(jnp.bfloat16), grad_total.astype(jnp.bfloat16))


def solution(mesh):
    dp_size = mesh.shape["dp"]
    paired = mesh.shape["tensor"] == 1 and dp_size >= 8 and dp_size & (dp_size - 1) == 0
    placed = (
        P("dp", None),
        P("dp", None),
        P("dp", None),
        P(),
        P(),
        P(),
        P("dp", "tensor"),
        P("dp", "tensor"),
        P("tensor", "dp"),
        P("dp", None, "tensor"),
        P("dp", None, "tensor"),
        P("dp", "tensor", None),
    )

    def body(*operands):
        return (paired_shards if paired else shards)(*operands)

    return jax.shard_map(
        body,
        mesh=mesh,
        in_specs=placed,
        out_specs=(P("dp", "tensor"), P("dp", "tensor")),
        check_vma=False,
    )
```

```python
import jax
import jax.numpy as jnp
from jax import lax
from jax.experimental import pallas as pl
from jax.experimental.pallas import tpu as pltpu
from jax.sharding import PartitionSpec as P


CAP = 9


def silu_pair(pre_gate):
    sigmoid_val = 1.0 / (1.0 + jnp.exp(-pre_gate))
    return (pre_gate * sigmoid_val, sigmoid_val * (1.0 + pre_gate * (1.0 - sigmoid_val)))


def contract_last(left, right):
    return lax.dot_general(
        left, right, (((1,), (1,)), ((), ())), preferred_element_type=jnp.float32
    )


def expert_block(rows_in, rows_cot, w_gate, w_up, w_down):
    pre_gate = jnp.dot(rows_in, w_gate, preferred_element_type=jnp.float32)
    pre_up = jnp.dot(rows_in, w_up, preferred_element_type=jnp.float32)
    active, derivative = silu_pair(pre_gate)
    hidden = (active * pre_up).astype(jnp.bfloat16)
    result = jnp.dot(hidden, w_down, preferred_element_type=jnp.float32)
    grad_hidden = contract_last(rows_cot, w_down)
    grad_gate = (grad_hidden * pre_up * derivative).astype(jnp.bfloat16)
    grad_up = (grad_hidden * active).astype(jnp.bfloat16)
    backward = contract_last(grad_gate, w_gate) + contract_last(grad_up, w_up)
    return (result, backward)


def expert_batch(rows_in, rows_cot, w_gate, w_up, w_down):
    pre_gate = jnp.einsum("slcd,ldf->slcf", rows_in, w_gate, preferred_element_type=jnp.float32)
    pre_up = jnp.einsum("slcd,ldf->slcf", rows_in, w_up, preferred_element_type=jnp.float32)
    active, derivative = silu_pair(pre_gate)
    hidden = (active * pre_up).astype(jnp.bfloat16)
    result = jnp.einsum(
        "slcf,lfd->slcd", hidden, w_down, preferred_element_type=jnp.float32
    ).astype(jnp.bfloat16)
    grad_hidden = jnp.einsum("slcd,lfd->slcf", rows_cot, w_down, preferred_element_type=jnp.float32)
    grad_gate = (grad_hidden * pre_up * derivative).astype(jnp.bfloat16)
    grad_up = (grad_hidden * active).astype(jnp.bfloat16)
    grad_both = jnp.concatenate([grad_gate, grad_up], axis=3)
    weight_both = jnp.concatenate([w_gate, w_up], axis=2)
    backward = jnp.einsum(
        "slcf,ldf->slcd", grad_both, weight_both, preferred_element_type=jnp.float32
    )
    return (result, backward.astype(jnp.bfloat16))


def shards(
    tokens,
    grad_out,
    route_ids,
    expert_map,
    router,
    shared_gate,
    sh_gate,
    sh_up,
    sh_down,
    ex_gate,
    ex_up,
    ex_down,
):
    tok_dev, width = tokens.shape
    top_count = route_ids.shape[1]
    expert_count = router.shape[1]
    dp_size = lax.axis_size("dp")
    tensor_size = lax.axis_size("tensor")
    tensor_rank = lax.axis_index("tensor")
    local_slots = ex_gate.shape[0]
    col_width = width // tensor_size
    col_start = tensor_rank * col_width
    buffer_rows = dp_size * local_slots * CAP
    slot_rows = local_slots * CAP
    flat_ids = route_ids.reshape(-1)
    chosen = (flat_ids[:, None] == jnp.arange(expert_count, dtype=jnp.int32)[None, :]).astype(
        jnp.int32
    )
    earlier = jnp.sum((jnp.cumsum(chosen, axis=0) - chosen) * chosen, axis=1)
    slot_of = jnp.sum(chosen * expert_map[None, :], axis=1)
    position = slot_of * CAP + earlier
    token_index = jnp.arange(tok_dev * top_count, dtype=jnp.int32) // top_count
    source_rows = jnp.full((buffer_rows,), tok_dev, jnp.int32).at[position].set(token_index)

    def fetch_rows(table):
        padded = jnp.concatenate([table, jnp.zeros((1, table.shape[1]), table.dtype)], axis=0)
        return jnp.take(padded, source_rows, axis=0)

    send_in = fetch_rows(tokens).reshape(dp_size, slot_rows, width)
    send_cot = fetch_rows(grad_out).reshape(dp_size, slot_rows, width)
    got_in = lax.all_to_all(send_in, "dp", split_axis=0, concat_axis=0, tiled=True)
    got_cot = lax.all_to_all(send_cot, "dp", split_axis=0, concat_axis=0, tiled=True)
    grid_shape = (dp_size, local_slots, CAP, width)
    result, backward = expert_batch(
        got_in.reshape(grid_shape), got_cot.reshape(grid_shape), ex_gate, ex_up, ex_down
    )
    came_out = lax.all_to_all(
        result.reshape(dp_size, slot_rows, width), "dp", split_axis=0, concat_axis=0, tiled=True
    )
    came_back = lax.all_to_all(
        backward.reshape(dp_size, slot_rows, width), "dp", split_axis=0, concat_axis=0, tiled=True
    )
    routed_out = came_out.reshape(buffer_rows, width)
    routed_back = came_back.reshape(buffer_rows, width)
    weights = (
        lax.all_gather(sh_gate, "dp", axis=0, tiled=True),
        lax.all_gather(sh_up, "dp", axis=0, tiled=True),
        lax.all_gather(sh_down, "dp", axis=1, tiled=True),
    )
    full_gate, full_up, full_down = weights
    sh_out, sh_back = expert_block(tokens, grad_out, full_gate, full_up, full_down)
    routed_width = routed_out.shape[1]
    expert_out = jnp.take(routed_out, position, axis=0).reshape(tok_dev, top_count, routed_width)
    expert_back = jnp.take(routed_back, position, axis=0).reshape(tok_dev, top_count, routed_width)
    logits = jnp.dot(tokens, router, preferred_element_type=jnp.float32)
    exp_logit = jnp.exp(logits)
    prob_table = exp_logit / jnp.sum(exp_logit, axis=1, keepdims=True)
    picked = chosen.reshape(tok_dev, top_count, expert_count).astype(jnp.float32)
    gate_weights = jnp.sum(picked * prob_table[:, None, :], axis=2)
    shared_scale = 1.0 / (
        1.0 + jnp.exp(-jnp.dot(tokens, shared_gate, preferred_element_type=jnp.float32))
    )
    shared_part = jnp.sum(grad_out.astype(jnp.float32) * sh_out, axis=1)
    dots_part = jnp.einsum("td,tkd->tk", grad_out, expert_out, preferred_element_type=jnp.float32)
    mixed_part = (
        jnp.sum(gate_weights[:, :, None] * expert_out.astype(jnp.float32), axis=1)
        + shared_scale[:, None] * sh_out
    )
    grad_part = (
        jnp.sum(gate_weights[:, :, None] * expert_back.astype(jnp.float32), axis=1)
        + shared_scale[:, None] * sh_back
    )
    out_dots, shared_dots = lax.psum((dots_part, shared_part), "tensor")
    mixed_cols, grad_cols = (
        lax.psum_scatter(mixed_part, "tensor", scatter_dimension=1, tiled=True),
        lax.psum_scatter(grad_part, "tensor", scatter_dimension=1, tiled=True),
    )
    grad_prob = jnp.sum(picked * out_dots[:, :, None], axis=1)
    dlogits = prob_table * (grad_prob - jnp.sum(gate_weights * out_dots, axis=1, keepdims=True))
    router_cols = lax.dynamic_slice_in_dim(router, col_start, col_width, 0).astype(jnp.float32)
    grad_router = lax.dot_general(
        dlogits,
        router_cols,
        (((1,), (1,)), ((), ())),
        precision=lax.Precision.HIGHEST,
        preferred_element_type=jnp.float32,
    )
    gate_cols = lax.dynamic_slice_in_dim(shared_gate, col_start, col_width, 0).astype(jnp.float32)
    slope_term = shared_dots * shared_scale * (1.0 - shared_scale)
    grad_total = grad_cols + grad_router + slope_term[:, None] * gate_cols[None, :]
    return (mixed_cols.astype(jnp.bfloat16), grad_total.astype(jnp.bfloat16))


def dot32(left, right):
    return jnp.dot(left, right, preferred_element_type=jnp.float32)


def expert_hidden(rows_in, w_gate, w_up):
    pre_gate = jnp.einsum("slcd,ldf->slcf", rows_in, w_gate, preferred_element_type=jnp.float32)
    pre_up = jnp.einsum("slcd,ldf->slcf", rows_in, w_up, preferred_element_type=jnp.float32)
    return pre_gate, pre_up


def assemble_kernel(order_ref, stacks, targets):
    first = 0
    for source, low in stacks:
        blocks, _, rows, _ = source.shape
        for j in range(blocks):
            for w, target in enumerate(targets):
                target[order_ref[first + j], low : low + rows, :] = source[j, w]
        first += blocks


def assemble(order, stacks, lows, shape):
    def kernel(order_ref, *refs):
        assemble_kernel(order_ref, list(zip(refs[:-3], lows)), refs[-3:])

    size = 3 * 2 * shape[0] * shape[1] * shape[2]
    return pl.pallas_call(
        kernel,
        in_specs=[pl.BlockSpec(memory_space=pltpu.SMEM)]
        + [pl.BlockSpec(memory_space=pltpu.VMEM)] * len(stacks),
        out_specs=[pl.BlockSpec(memory_space=pltpu.VMEM)] * 3,
        out_shape=[jax.ShapeDtypeStruct(shape, stacks[0].dtype)] * 3,
        cost_estimate=pl.CostEstimate(
            flops=100 * size, bytes_accessed=2 * size, transcendentals=0
        ),
    )(order, *stacks)


def after(value, *others):
    return lax.optimization_barrier((value,) + others)[0]


def paired_shards(
    tokens,
    grad_out,
    route_ids,
    expert_map,
    router,
    shared_gate,
    sh_gate,
    sh_up,
    sh_down,
    ex_gate,
    ex_up,
    ex_down,
):
    tok_dev, width = tokens.shape
    top_count = route_ids.shape[1]
    expert_count = router.shape[1]
    dp_size = lax.axis_size("dp")
    local_slots = ex_gate.shape[0]
    half_size = dp_size // 2
    lanes = half_size // 2
    lane_bits = lanes.bit_length() - 1
    rows_main = 4 * CAP // 8 * 8
    rows_last = 4 * CAP - rows_main
    rows_shared = -(-rows_last * local_slots // 8) * 8
    rows_lane = local_slots * rows_main + rows_shared
    rows_all = lanes * rows_lane
    me = lax.axis_index("dp")
    half = me // half_size
    lane = (me % half_size) // 2
    core = me % 2
    pair_half = [(i, i ^ half_size) for i in range(dp_size)]
    pair_core = [(i, i ^ 1) for i in range(dp_size)]
    lane_groups = [
        [h * half_size + 2 * n + c for n in range(lanes)] for h in range(2) for c in range(2)
    ]

    def across(value, pairs):
        return lax.ppermute(value, "dp", pairs)

    def exchange(value):
        return lax.all_to_all(
            value, "dp", split_axis=0, concat_axis=0, tiled=True, axis_index_groups=lane_groups
        )

    tokens_far = across(tokens, pair_half)
    grads_far = across(after(grad_out, tokens_far), pair_half)
    tokens_two = jnp.concatenate([tokens, tokens_far], axis=0)
    grads_two = jnp.concatenate([grad_out, grads_far], axis=0)

    chosen = (
        route_ids[:, :, None] == jnp.arange(expert_count, dtype=jnp.int32)[None, None, :]
    ).astype(jnp.float32)
    named = jnp.sum(chosen, axis=1)
    before = (
        jnp.arange(tok_dev, dtype=jnp.int32)[:, None]
        > jnp.arange(tok_dev, dtype=jnp.int32)[None, :]
    ).astype(jnp.bfloat16)
    earlier = dot32(before, named.astype(jnp.bfloat16))
    rank = jnp.sum(chosen * earlier[:, None, :], axis=2)
    slot = jnp.sum(chosen * expert_map.astype(jnp.float32)[None, None, :], axis=2)
    logits = dot32(tokens, router)
    exp_logit = jnp.exp(logits)
    prob_table = exp_logit / jnp.sum(exp_logit, axis=1, keepdims=True)
    gate_weights = jnp.sum(chosen * prob_table[:, None, :], axis=2)
    shared_scale = 1.0 / (1.0 + jnp.exp(-dot32(tokens, shared_gate)))
    meta = jnp.concatenate([slot, rank, gate_weights, shared_scale[:, None]], axis=1)
    meta_two = jnp.concatenate([meta, across(meta, pair_half)], axis=0)
    meta_all = jnp.concatenate([meta_two, across(meta_two, pair_core)], axis=0)
    tokens_all = jnp.concatenate([tokens_two, across(tokens_two, pair_core)], axis=0)
    grads_all = jnp.concatenate([grads_two, across(grads_two, pair_core)], axis=0)
    tok_all = 4 * tok_dev

    slot_all = meta_all[:, :top_count].astype(jnp.int32)
    rank_all = meta_all[:, top_count : 2 * top_count].astype(jnp.int32)
    gates_all = meta_all[:, 2 * top_count : 3 * top_count]
    scale_all = meta_all[:, 3 * top_count :]
    holder = slot_all // local_slots
    block = jnp.arange(tok_all, dtype=jnp.int32)[:, None] // tok_dev
    inside = block * CAP + rank_all
    local = slot_all % local_slots
    inside = jnp.where(
        inside < rows_main,
        local * rows_main + inside,
        local_slots * rows_main + local * rows_last + inside - rows_main,
    )
    row_at = ((holder % half_size) // 2) * rows_lane + inside
    row_at = jnp.where((holder // half_size == half) & (holder % 2 == core), row_at, -1)
    row_ids = jnp.arange(rows_all, dtype=jnp.int32)
    pick_rows = jnp.sum(
        (row_at.T[:, None, :] == row_ids[None, :, None]).astype(jnp.float32), axis=0
    ).astype(jnp.bfloat16)
    hit = row_at[:, :, None] == row_ids[None, None, :]
    place = jnp.sum(jnp.where(hit, gates_all[:, :, None], 0.0), axis=1).astype(jnp.bfloat16)

    def dispatch(table):
        rows = dot32(pick_rows, table).astype(jnp.bfloat16)
        got = exchange(rows.reshape(lanes, rows_lane, width))
        main = got[:, : local_slots * rows_main].reshape(lanes, local_slots, rows_main, width)
        last = jnp.broadcast_to(
            got[:, None, local_slots * rows_main :], (lanes, local_slots, rows_shared, width)
        )
        return jnp.concatenate([main, last], axis=2)

    def pack(rows):
        main = rows[:, :, :rows_main].reshape(lanes, local_slots * rows_main, width)
        owner = jnp.arange(rows_shared, dtype=jnp.int32)[None, :, None] // max(rows_last, 1)
        last = rows[:, 0, rows_main:]
        for local in range(1, local_slots):
            last = jnp.where(owner == local, rows[:, local, rows_main:], last)
        return jnp.concatenate([main, last], axis=1)

    def give_back(sent):
        return exchange(sent).reshape(rows_all, width)

    got_in = dispatch(tokens_all)
    got_cot = dispatch(grads_all)

    hidden_all = sh_gate.shape[1]
    quarter = hidden_all // 4
    quarter_pad = -(-quarter // 128) * 128
    shard = jnp.stack([sh_gate, sh_up, sh_down.T]).reshape(3, width // dp_size, 4, quarter)
    shard = jnp.pad(shard, ((0, 0), (0, 0), (0, 0), (0, quarter_pad - quarter)))
    shard = shard.transpose(2, 0, 1, 3).reshape(2, 2, 3, width // dp_size, quarter_pad)
    kept = lax.dynamic_index_in_dim(shard, core, 0, keepdims=False)
    sent = lax.dynamic_index_in_dim(shard, 1 - core, 0, keepdims=False)
    came = across(sent, pair_core)
    both = jnp.where(
        core == 0, jnp.concatenate([kept, came], axis=2), jnp.concatenate([came, kept], axis=2)
    )
    own_rows = lax.dynamic_index_in_dim(both, half, 0, keepdims=False)
    far_rows = lax.dynamic_index_in_dim(both, 1 - half, 0, keepdims=False)
    far_rows = across(after(far_rows, grads_far), pair_half)

    def lane_hop(value, bit):
        return across(value, [(i, i ^ (2 * bit)) for i in range(dp_size)])

    def spread(block):
        top = lanes // 2
        held_all = jnp.stack([block, lane_hop(block, top)])
        chains = max(lane_bits - 1, 1)
        rows = block.shape[1] // chains
        stacks, lows, sources = [], [], []
        for chain in range(chains):
            held, came_from = held_all[:, :, chain * rows : (chain + 1) * rows], [0, top]
            bits = [1 << ((chain + step) % chains) for step in range(lane_bits - 1)]
            for step, bit in enumerate(bits):
                received = lane_hop(held, bit)
                moved = [d ^ bit for d in came_from]
                if step == len(bits) - 1:
                    stacks += [held, received]
                    lows += [chain * rows] * 2
                    sources += came_from + moved
                else:
                    held = jnp.concatenate([held, received], axis=0)
                    came_from = came_from + moved
        return stacks, lows, sources

    pre_gate, pre_up = expert_hidden(got_in, ex_gate, ex_up)
    active, derivative = silu_pair(pre_gate)
    hidden, active, slope = lax.optimization_barrier(
        ((active * pre_up).astype(jnp.bfloat16), active, pre_up * derivative)
    )
    result = jnp.einsum(
        "slcf,lfd->slcd", hidden, ex_down, preferred_element_type=jnp.float32
    ).astype(jnp.bfloat16)
    sent_out = after(pack(result), place)
    routed_out = give_back(sent_out)
    got_cot = after(got_cot, sent_out)
    grad_hidden = jnp.einsum("slcd,lfd->slcf", got_cot, ex_down, preferred_element_type=jnp.float32)
    grad_gate = (grad_hidden * slope).astype(jnp.bfloat16)
    grad_up = (grad_hidden * active).astype(jnp.bfloat16)
    grad_both = jnp.concatenate([grad_gate, grad_up], axis=3)
    weight_both = jnp.concatenate([ex_gate, ex_up], axis=2)
    backward = jnp.einsum(
        "slcf,ldf->slcd", grad_both, weight_both, preferred_element_type=jnp.float32
    ).astype(jnp.bfloat16)
    routed_back = give_back(pack(backward))

    own_stacks, own_lows, sources = spread(own_rows)
    far_stacks, far_lows, _ = spread(far_rows)
    lanes_of = jnp.array(sources, jnp.int32) ^ lane
    order = jnp.concatenate([half * lanes + lanes_of, (1 - half) * lanes + lanes_of])
    full = assemble(
        order,
        own_stacks + far_stacks,
        own_lows + far_lows,
        (2 * lanes, own_rows.shape[1], quarter_pad),
    )
    full_gate, full_up, full_down = [f.reshape(width, quarter_pad) for f in full]

    sh_pre_gate = dot32(tokens_all, full_gate)
    sh_pre_up = dot32(tokens_all, full_up)
    sh_active, sh_derivative = silu_pair(sh_pre_gate)
    sh_hidden = (sh_active * sh_pre_up).astype(jnp.bfloat16)
    sh_out = contract_last(sh_hidden, full_down)
    mixed_part = dot32(place, routed_out) + scale_all * sh_out
    sh_grad_hidden = dot32(after(grads_all, mixed_part), full_down)
    sh_grad_gate = (sh_grad_hidden * sh_pre_up * sh_derivative).astype(jnp.bfloat16)
    sh_grad_up = (sh_grad_hidden * sh_active).astype(jnp.bfloat16)
    sh_back = contract_last(sh_grad_gate, full_gate) + contract_last(sh_grad_up, full_up)
    sh_back = lax.optimization_barrier(scale_all * sh_back)

    def collect(partial):
        sent = partial[2 * tok_dev :].astype(jnp.bfloat16)
        came = across(sent, pair_core).astype(jnp.float32)
        pair_sum = partial[: 2 * tok_dev] + came
        sent = pair_sum[tok_dev:].astype(jnp.bfloat16)
        return pair_sum[:tok_dev] + across(sent, pair_half).astype(jnp.float32)

    mixed = collect(mixed_part)
    all_dots = contract_last(grads_all, routed_out)
    dots_part = jnp.sum(jnp.where(hit, all_dots[:, None, :], 0.0), axis=2)
    shared_part = jnp.sum(grads_all.astype(jnp.float32) * sh_out, axis=1, keepdims=True)
    scalars = jnp.concatenate([dots_part, shared_part], axis=1)
    scalars = scalars[: 2 * tok_dev] + across(scalars[2 * tok_dev :], pair_core)
    scalars = scalars[:tok_dev] + across(scalars[tok_dev:], pair_half)
    out_dots = scalars[:, :top_count]
    shared_dots = scalars[:, top_count]
    grad_part = collect(dot32(place, routed_back) + sh_back)

    grad_prob = jnp.sum(chosen * out_dots[:, :, None], axis=1)
    dlogits = prob_table * (grad_prob - jnp.sum(gate_weights * out_dots, axis=1, keepdims=True))
    grad_router = lax.dot_general(
        dlogits,
        router.astype(jnp.float32),
        (((1,), (1,)), ((), ())),
        precision=lax.Precision.HIGHEST,
        preferred_element_type=jnp.float32,
    )
    slope_term = shared_dots * shared_scale * (1.0 - shared_scale)
    grad_total = (
        grad_part + grad_router + slope_term[:, None] * shared_gate.astype(jnp.float32)[None, :]
    )
    return (mixed.astype(jnp.bfloat16), grad_total.astype(jnp.bfloat16))


def solution(mesh):
    dp_size = mesh.shape["dp"]
    paired = mesh.shape["tensor"] == 1 and dp_size >= 8 and dp_size & (dp_size - 1) == 0
    placed = (
        P("dp", None),
        P("dp", None),
        P("dp", None),
        P(),
        P(),
        P(),
        P("dp", "tensor"),
        P("dp", "tensor"),
        P("tensor", "dp"),
        P("dp", None, "tensor"),
        P("dp", None, "tensor"),
        P("dp", "tensor", None),
    )

    def body(*operands):
        return (paired_shards if paired else shards)(*operands)

    return jax.shard_map(
        body,
        mesh=mesh,
        in_specs=placed,
        out_specs=(P("dp", "tensor"), P("dp", "tensor")),
        check_vma=False,
    )
```

```python
import jax
import jax.numpy as jnp
from jax import lax
from jax.experimental import pallas as pl
from jax.experimental.pallas import tpu as pltpu
from jax.sharding import PartitionSpec as P


CAP = 9


def silu_pair(pre_gate):
    sigmoid_val = 1.0 / (1.0 + jnp.exp(-pre_gate))
    return (pre_gate * sigmoid_val, sigmoid_val * (1.0 + pre_gate * (1.0 - sigmoid_val)))


def contract_last(left, right):
    return lax.dot_general(
        left, right, (((1,), (1,)), ((), ())), preferred_element_type=jnp.float32
    )


def expert_block(rows_in, rows_cot, w_gate, w_up, w_down):
    pre_gate = jnp.dot(rows_in, w_gate, preferred_element_type=jnp.float32)
    pre_up = jnp.dot(rows_in, w_up, preferred_element_type=jnp.float32)
    active, derivative = silu_pair(pre_gate)
    hidden = (active * pre_up).astype(jnp.bfloat16)
    result = jnp.dot(hidden, w_down, preferred_element_type=jnp.float32)
    grad_hidden = contract_last(rows_cot, w_down)
    grad_gate = (grad_hidden * pre_up * derivative).astype(jnp.bfloat16)
    grad_up = (grad_hidden * active).astype(jnp.bfloat16)
    backward = contract_last(grad_gate, w_gate) + contract_last(grad_up, w_up)
    return (result, backward)


def expert_batch(rows_in, rows_cot, w_gate, w_up, w_down):
    pre_gate = jnp.einsum("slcd,ldf->slcf", rows_in, w_gate, preferred_element_type=jnp.float32)
    pre_up = jnp.einsum("slcd,ldf->slcf", rows_in, w_up, preferred_element_type=jnp.float32)
    active, derivative = silu_pair(pre_gate)
    hidden = (active * pre_up).astype(jnp.bfloat16)
    result = jnp.einsum(
        "slcf,lfd->slcd", hidden, w_down, preferred_element_type=jnp.float32
    ).astype(jnp.bfloat16)
    grad_hidden = jnp.einsum("slcd,lfd->slcf", rows_cot, w_down, preferred_element_type=jnp.float32)
    grad_gate = (grad_hidden * pre_up * derivative).astype(jnp.bfloat16)
    grad_up = (grad_hidden * active).astype(jnp.bfloat16)
    grad_both = jnp.concatenate([grad_gate, grad_up], axis=3)
    weight_both = jnp.concatenate([w_gate, w_up], axis=2)
    backward = jnp.einsum(
        "slcf,ldf->slcd", grad_both, weight_both, preferred_element_type=jnp.float32
    )
    return (result, backward.astype(jnp.bfloat16))


def shards(
    tokens,
    grad_out,
    route_ids,
    expert_map,
    router,
    shared_gate,
    sh_gate,
    sh_up,
    sh_down,
    ex_gate,
    ex_up,
    ex_down,
):
    tok_dev, width = tokens.shape
    top_count = route_ids.shape[1]
    expert_count = router.shape[1]
    dp_size = lax.axis_size("dp")
    tensor_size = lax.axis_size("tensor")
    tensor_rank = lax.axis_index("tensor")
    local_slots = ex_gate.shape[0]
    col_width = width // tensor_size
    col_start = tensor_rank * col_width
    buffer_rows = dp_size * local_slots * CAP
    slot_rows = local_slots * CAP
    flat_ids = route_ids.reshape(-1)
    chosen = (flat_ids[:, None] == jnp.arange(expert_count, dtype=jnp.int32)[None, :]).astype(
        jnp.int32
    )
    earlier = jnp.sum((jnp.cumsum(chosen, axis=0) - chosen) * chosen, axis=1)
    slot_of = jnp.sum(chosen * expert_map[None, :], axis=1)
    position = slot_of * CAP + earlier
    token_index = jnp.arange(tok_dev * top_count, dtype=jnp.int32) // top_count
    source_rows = jnp.full((buffer_rows,), tok_dev, jnp.int32).at[position].set(token_index)

    def fetch_rows(table):
        padded = jnp.concatenate([table, jnp.zeros((1, table.shape[1]), table.dtype)], axis=0)
        return jnp.take(padded, source_rows, axis=0)

    send_in = fetch_rows(tokens).reshape(dp_size, slot_rows, width)
    send_cot = fetch_rows(grad_out).reshape(dp_size, slot_rows, width)
    got_in = lax.all_to_all(send_in, "dp", split_axis=0, concat_axis=0, tiled=True)
    got_cot = lax.all_to_all(send_cot, "dp", split_axis=0, concat_axis=0, tiled=True)
    grid_shape = (dp_size, local_slots, CAP, width)
    result, backward = expert_batch(
        got_in.reshape(grid_shape), got_cot.reshape(grid_shape), ex_gate, ex_up, ex_down
    )
    came_out = lax.all_to_all(
        result.reshape(dp_size, slot_rows, width), "dp", split_axis=0, concat_axis=0, tiled=True
    )
    came_back = lax.all_to_all(
        backward.reshape(dp_size, slot_rows, width), "dp", split_axis=0, concat_axis=0, tiled=True
    )
    routed_out = came_out.reshape(buffer_rows, width)
    routed_back = came_back.reshape(buffer_rows, width)
    weights = (
        lax.all_gather(sh_gate, "dp", axis=0, tiled=True),
        lax.all_gather(sh_up, "dp", axis=0, tiled=True),
        lax.all_gather(sh_down, "dp", axis=1, tiled=True),
    )
    full_gate, full_up, full_down = weights
    sh_out, sh_back = expert_block(tokens, grad_out, full_gate, full_up, full_down)
    routed_width = routed_out.shape[1]
    expert_out = jnp.take(routed_out, position, axis=0).reshape(tok_dev, top_count, routed_width)
    expert_back = jnp.take(routed_back, position, axis=0).reshape(tok_dev, top_count, routed_width)
    logits = jnp.dot(tokens, router, preferred_element_type=jnp.float32)
    exp_logit = jnp.exp(logits)
    prob_table = exp_logit / jnp.sum(exp_logit, axis=1, keepdims=True)
    picked = chosen.reshape(tok_dev, top_count, expert_count).astype(jnp.float32)
    gate_weights = jnp.sum(picked * prob_table[:, None, :], axis=2)
    shared_scale = 1.0 / (
        1.0 + jnp.exp(-jnp.dot(tokens, shared_gate, preferred_element_type=jnp.float32))
    )
    shared_part = jnp.sum(grad_out.astype(jnp.float32) * sh_out, axis=1)
    dots_part = jnp.einsum("td,tkd->tk", grad_out, expert_out, preferred_element_type=jnp.float32)
    mixed_part = (
        jnp.sum(gate_weights[:, :, None] * expert_out.astype(jnp.float32), axis=1)
        + shared_scale[:, None] * sh_out
    )
    grad_part = (
        jnp.sum(gate_weights[:, :, None] * expert_back.astype(jnp.float32), axis=1)
        + shared_scale[:, None] * sh_back
    )
    out_dots, shared_dots = lax.psum((dots_part, shared_part), "tensor")
    mixed_cols, grad_cols = (
        lax.psum_scatter(mixed_part, "tensor", scatter_dimension=1, tiled=True),
        lax.psum_scatter(grad_part, "tensor", scatter_dimension=1, tiled=True),
    )
    grad_prob = jnp.sum(picked * out_dots[:, :, None], axis=1)
    dlogits = prob_table * (grad_prob - jnp.sum(gate_weights * out_dots, axis=1, keepdims=True))
    router_cols = lax.dynamic_slice_in_dim(router, col_start, col_width, 0).astype(jnp.float32)
    grad_router = lax.dot_general(
        dlogits,
        router_cols,
        (((1,), (1,)), ((), ())),
        precision=lax.Precision.HIGHEST,
        preferred_element_type=jnp.float32,
    )
    gate_cols = lax.dynamic_slice_in_dim(shared_gate, col_start, col_width, 0).astype(jnp.float32)
    slope_term = shared_dots * shared_scale * (1.0 - shared_scale)
    grad_total = grad_cols + grad_router + slope_term[:, None] * gate_cols[None, :]
    return (mixed_cols.astype(jnp.bfloat16), grad_total.astype(jnp.bfloat16))


def dot32(left, right):
    return jnp.dot(left, right, preferred_element_type=jnp.float32)


def expert_hidden(rows_in, w_gate, w_up):
    pre_gate = jnp.einsum("slcd,ldf->slcf", rows_in, w_gate, preferred_element_type=jnp.float32)
    pre_up = jnp.einsum("slcd,ldf->slcf", rows_in, w_up, preferred_element_type=jnp.float32)
    return pre_gate, pre_up


def assemble_kernel(order_ref, stacks, targets):
    first = 0
    for source, low in stacks:
        blocks, _, rows, _ = source.shape
        cols = source.shape[3]
        for j in range(blocks):
            at = order_ref[first + j]
            targets[0][at, low : low + rows, :cols] = source[j, 0]
            targets[0][at, low : low + rows, cols:] = source[j, 1]
            targets[1][at, low : low + rows, :] = source[j, 2]
        first += blocks


def assemble(order, stacks, lows, shape):
    def kernel(order_ref, *refs):
        assemble_kernel(order_ref, list(zip(refs[:-2], lows)), refs[-2:])

    size = 3 * 2 * shape[0] * shape[1] * shape[2]
    return pl.pallas_call(
        kernel,
        in_specs=[pl.BlockSpec(memory_space=pltpu.SMEM)]
        + [pl.BlockSpec(memory_space=pltpu.VMEM)] * len(stacks),
        out_specs=[pl.BlockSpec(memory_space=pltpu.VMEM)] * 2,
        out_shape=[
            jax.ShapeDtypeStruct(shape[:2] + (2 * shape[2],), stacks[0].dtype),
            jax.ShapeDtypeStruct(shape, stacks[0].dtype),
        ],
        cost_estimate=pl.CostEstimate(
            flops=100 * size, bytes_accessed=2 * size, transcendentals=0
        ),
    )(order, *stacks)


def after(value, *others):
    return lax.optimization_barrier((value,) + others)[0]


def paired_shards(
    tokens,
    grad_out,
    route_ids,
    expert_map,
    router,
    shared_gate,
    sh_gate,
    sh_up,
    sh_down,
    ex_gate,
    ex_up,
    ex_down,
):
    tok_dev, width = tokens.shape
    top_count = route_ids.shape[1]
    expert_count = router.shape[1]
    dp_size = lax.axis_size("dp")
    local_slots = ex_gate.shape[0]
    half_size = dp_size // 2
    lanes = half_size // 2
    lane_bits = lanes.bit_length() - 1
    rows_main = 4 * CAP // 8 * 8
    rows_last = 4 * CAP - rows_main
    rows_shared = -(-rows_last * local_slots // 8) * 8
    rows_lane = local_slots * rows_main + rows_shared
    rows_all = lanes * rows_lane
    me = lax.axis_index("dp")
    half = me // half_size
    lane = (me % half_size) // 2
    core = me % 2
    pair_half = [(i, i ^ half_size) for i in range(dp_size)]
    pair_core = [(i, i ^ 1) for i in range(dp_size)]
    lane_groups = [
        [h * half_size + 2 * n + c for n in range(lanes)] for h in range(2) for c in range(2)
    ]

    def across(value, pairs):
        return lax.ppermute(value, "dp", pairs)

    def exchange(value):
        return lax.all_to_all(
            value, "dp", split_axis=0, concat_axis=0, tiled=True, axis_index_groups=lane_groups
        )

    tokens_far = across(tokens, pair_half)
    grads_far = across(after(grad_out, tokens_far), pair_half)
    tokens_two = jnp.concatenate([tokens, tokens_far], axis=0)
    grads_two = jnp.concatenate([grad_out, grads_far], axis=0)

    chosen = (
        route_ids[:, :, None] == jnp.arange(expert_count, dtype=jnp.int32)[None, None, :]
    ).astype(jnp.float32)
    named = jnp.sum(chosen, axis=1)
    before = (
        jnp.arange(tok_dev, dtype=jnp.int32)[:, None]
        > jnp.arange(tok_dev, dtype=jnp.int32)[None, :]
    ).astype(jnp.bfloat16)
    earlier = dot32(before, named.astype(jnp.bfloat16))
    rank = jnp.sum(chosen * earlier[:, None, :], axis=2)
    slot = jnp.sum(chosen * expert_map.astype(jnp.float32)[None, None, :], axis=2)
    logits = dot32(tokens, router)
    exp_logit = jnp.exp(logits)
    prob_table = exp_logit / jnp.sum(exp_logit, axis=1, keepdims=True)
    gate_weights = jnp.sum(chosen * prob_table[:, None, :], axis=2)
    shared_scale = 1.0 / (1.0 + jnp.exp(-dot32(tokens, shared_gate)))
    meta = jnp.concatenate([slot, rank, gate_weights, shared_scale[:, None]], axis=1)
    meta_two = jnp.concatenate([meta, across(meta, pair_half)], axis=0)
    meta_all = jnp.concatenate([meta_two, across(meta_two, pair_core)], axis=0)
    tokens_all = jnp.concatenate([tokens_two, across(tokens_two, pair_core)], axis=0)
    grads_all = jnp.concatenate([grads_two, across(grads_two, pair_core)], axis=0)
    tok_all = 4 * tok_dev

    slot_all = meta_all[:, :top_count].astype(jnp.int32)
    rank_all = meta_all[:, top_count : 2 * top_count].astype(jnp.int32)
    gates_all = meta_all[:, 2 * top_count : 3 * top_count]
    scale_all = meta_all[:, 3 * top_count :]
    holder = slot_all // local_slots
    block = jnp.arange(tok_all, dtype=jnp.int32)[:, None] // tok_dev
    inside = block * CAP + rank_all
    local = slot_all % local_slots
    inside = jnp.where(
        inside < rows_main,
        local * rows_main + inside,
        local_slots * rows_main + local * rows_last + inside - rows_main,
    )
    row_at = ((holder % half_size) // 2) * rows_lane + inside
    row_at = jnp.where((holder // half_size == half) & (holder % 2 == core), row_at, -1)
    row_ids = jnp.arange(rows_all, dtype=jnp.int32)
    pick_rows = jnp.sum(
        (row_at.T[:, None, :] == row_ids[None, :, None]).astype(jnp.float32), axis=0
    ).astype(jnp.bfloat16)
    hit = row_at[:, :, None] == row_ids[None, None, :]
    place = jnp.sum(jnp.where(hit, gates_all[:, :, None], 0.0), axis=1).astype(jnp.bfloat16)

    def dispatch(table):
        rows = dot32(pick_rows, table).astype(jnp.bfloat16)
        got = exchange(rows.reshape(lanes, rows_lane, width))
        main = got[:, : local_slots * rows_main].reshape(lanes, local_slots, rows_main, width)
        last = jnp.broadcast_to(
            got[:, None, local_slots * rows_main :], (lanes, local_slots, rows_shared, width)
        )
        return jnp.concatenate([main, last], axis=2)

    def pack(rows):
        main = rows[:, :, :rows_main].reshape(lanes, local_slots * rows_main, width)
        owner = jnp.arange(rows_shared, dtype=jnp.int32)[None, :, None] // max(rows_last, 1)
        last = rows[:, 0, rows_main:]
        for local in range(1, local_slots):
            last = jnp.where(owner == local, rows[:, local, rows_main:], last)
        return jnp.concatenate([main, last], axis=1)

    def give_back(sent):
        return exchange(sent).reshape(rows_all, width)

    got_in = dispatch(tokens_all)
    got_cot = dispatch(grads_all)

    hidden_all = sh_gate.shape[1]
    quarter = hidden_all // 4
    quarter_pad = -(-quarter // 128) * 128
    shard = jnp.stack([sh_gate, sh_up, sh_down.T]).reshape(3, width // dp_size, 4, quarter)
    shard = jnp.pad(shard, ((0, 0), (0, 0), (0, 0), (0, quarter_pad - quarter)))
    shard = shard.transpose(2, 0, 1, 3).reshape(2, 2, 3, width // dp_size, quarter_pad)
    kept = lax.dynamic_index_in_dim(shard, core, 0, keepdims=False)
    sent = lax.dynamic_index_in_dim(shard, 1 - core, 0, keepdims=False)
    came = across(sent, pair_core)
    both = jnp.where(
        core == 0, jnp.concatenate([kept, came], axis=2), jnp.concatenate([came, kept], axis=2)
    )
    own_rows = lax.dynamic_index_in_dim(both, half, 0, keepdims=False)
    far_rows = lax.dynamic_index_in_dim(both, 1 - half, 0, keepdims=False)
    far_rows = across(after(far_rows, grads_far), pair_half)

    def lane_hop(value, bit):
        return across(value, [(i, i ^ (2 * bit)) for i in range(dp_size)])

    def spread(block):
        top = lanes // 2
        held_all = jnp.stack([block, lane_hop(block, top)])
        chains = max(lane_bits - 1, 1)
        rows = block.shape[1] // chains
        stacks, lows, sources = [], [], []
        for chain in range(chains):
            held, came_from = held_all[:, :, chain * rows : (chain + 1) * rows], [0, top]
            bits = [1 << ((chain + step) % chains) for step in range(lane_bits - 1)]
            for step, bit in enumerate(bits):
                received = lane_hop(held, bit)
                moved = [d ^ bit for d in came_from]
                if step == len(bits) - 1:
                    stacks += [held, received]
                    lows += [chain * rows] * 2
                    sources += came_from + moved
                else:
                    held = jnp.concatenate([held, received], axis=0)
                    came_from = came_from + moved
        return stacks, lows, sources

    pre_gate, pre_up = expert_hidden(got_in, ex_gate, ex_up)
    active, derivative = silu_pair(pre_gate)
    hidden, active, slope = lax.optimization_barrier(
        ((active * pre_up).astype(jnp.bfloat16), active, pre_up * derivative)
    )
    result = jnp.einsum(
        "slcf,lfd->slcd", hidden, ex_down, preferred_element_type=jnp.float32
    ).astype(jnp.bfloat16)
    sent_out = after(pack(result), place)
    routed_out = give_back(sent_out)
    got_cot = after(got_cot, sent_out)
    grad_hidden = jnp.einsum("slcd,lfd->slcf", got_cot, ex_down, preferred_element_type=jnp.float32)
    grad_gate = (grad_hidden * slope).astype(jnp.bfloat16)
    grad_up = (grad_hidden * active).astype(jnp.bfloat16)
    grad_both = jnp.concatenate([grad_gate, grad_up], axis=3)
    weight_both = jnp.concatenate([ex_gate, ex_up], axis=2)
    backward = jnp.einsum(
        "slcf,ldf->slcd", grad_both, weight_both, preferred_element_type=jnp.float32
    ).astype(jnp.bfloat16)
    routed_back = give_back(pack(backward))

    own_stacks, own_lows, sources = spread(own_rows)
    far_stacks, far_lows, _ = spread(far_rows)
    lanes_of = jnp.array(sources, jnp.int32) ^ lane
    order = jnp.concatenate([half * lanes + lanes_of, (1 - half) * lanes + lanes_of])
    full = assemble(
        order,
        own_stacks + far_stacks,
        own_lows + far_lows,
        (2 * lanes, own_rows.shape[1], quarter_pad),
    )
    full_both, full_down = [f.reshape(width, -1) for f in full]

    mixed_routed = lax.optimization_barrier(dot32(place, routed_out))
    sh_pre = dot32(tokens_all, full_both)
    sh_pre_gate, sh_pre_up = sh_pre[:, :quarter_pad], sh_pre[:, quarter_pad:]
    sh_active, sh_derivative = silu_pair(sh_pre_gate)
    sh_hidden = (sh_active * sh_pre_up).astype(jnp.bfloat16)
    sh_out = contract_last(sh_hidden, full_down)
    mixed_part = mixed_routed + scale_all * sh_out
    sh_grad_hidden = dot32(after(grads_all, mixed_part), full_down)
    sh_grad_gate = (sh_grad_hidden * sh_pre_up * sh_derivative).astype(jnp.bfloat16)
    sh_grad_up = (sh_grad_hidden * sh_active).astype(jnp.bfloat16)
    sh_back = contract_last(jnp.concatenate([sh_grad_gate, sh_grad_up], axis=1), full_both)
    sh_back = lax.optimization_barrier(scale_all * sh_back)

    def collect(partial):
        sent = partial[2 * tok_dev :].astype(jnp.bfloat16)
        came = across(sent, pair_core).astype(jnp.float32)
        pair_sum = partial[: 2 * tok_dev] + came
        sent = pair_sum[tok_dev:].astype(jnp.bfloat16)
        return pair_sum[:tok_dev] + across(sent, pair_half).astype(jnp.float32)

    mixed = collect(mixed_part)
    all_dots = contract_last(grads_all, routed_out)
    dots_part = jnp.sum(jnp.where(hit, all_dots[:, None, :], 0.0), axis=2)
    shared_part = jnp.sum(grads_all.astype(jnp.float32) * sh_out, axis=1, keepdims=True)
    scalars = jnp.concatenate([dots_part, shared_part], axis=1)
    scalars = scalars[: 2 * tok_dev] + across(scalars[2 * tok_dev :], pair_core)
    scalars = scalars[:tok_dev] + across(scalars[tok_dev:], pair_half)
    out_dots = scalars[:, :top_count]
    shared_dots = scalars[:, top_count]
    grad_part = collect(dot32(place, routed_back) + sh_back)

    grad_prob = jnp.sum(chosen * out_dots[:, :, None], axis=1)
    dlogits = prob_table * (grad_prob - jnp.sum(gate_weights * out_dots, axis=1, keepdims=True))
    grad_router = lax.dot_general(
        dlogits,
        router.astype(jnp.float32),
        (((1,), (1,)), ((), ())),
        precision=lax.Precision.HIGHEST,
        preferred_element_type=jnp.float32,
    )
    slope_term = shared_dots * shared_scale * (1.0 - shared_scale)
    grad_total = (
        grad_part + grad_router + slope_term[:, None] * shared_gate.astype(jnp.float32)[None, :]
    )
    return (mixed.astype(jnp.bfloat16), grad_total.astype(jnp.bfloat16))


def solution(mesh):
    dp_size = mesh.shape["dp"]
    paired = mesh.shape["tensor"] == 1 and dp_size >= 8 and dp_size & (dp_size - 1) == 0
    placed = (
        P("dp", None),
        P("dp", None),
        P("dp", None),
        P(),
        P(),
        P(),
        P("dp", "tensor"),
        P("dp", "tensor"),
        P("tensor", "dp"),
        P("dp", None, "tensor"),
        P("dp", None, "tensor"),
        P("dp", "tensor", None),
    )

    def body(*operands):
        return (paired_shards if paired else shards)(*operands)

    return jax.shard_map(
        body,
        mesh=mesh,
        in_specs=placed,
        out_specs=(P("dp", "tensor"), P("dp", "tensor")),
        check_vma=False,
    )
```
